32 devices in a mesh: pair: 4 (over x, core), row: 8 (over z, y).
Axes of the slice: x: 2, y: 2, z: 4, core: 2. Of those that a mesh axis runs over, the one named last changes fastest.
Arguments:
- descriptors: bfloat16 [32, 2048, 256], P('pair', 'row'), parts along dimension 0, may hold values from -8 to 8
- counts: int32 [32], P('pair'), parts along dimension 0, may hold values from 512 to 2048
- pairs: int32 [16, 2], P('pair'), parts along dimension 0, may hold values from 0 to 7, as said below
- bin_score: float32 [1], replicated, may hold values from 0.5 to 2
Outputs:
- log_match: float32 [16, 2048, 2048], P('pair', 'row'), parts along dimension 0
- row_bins: float32 [16, 2048], P('pair', 'row'), parts along dimension 0
- col_bins: float32 [16, 2048], P('pair'), parts along dimension 0
The draws below stay inside these ranges and needn't reach their ends.
There are 4 independent parts, one for each index of `pair`. The reference program is written for one: setup_inputs(seed, part) draws one part's arguments, and reference() takes and returns one part's arrays. A program takes and returns all parts, laid end to end along the dimension named above; an argument that names none is the same for every part. Nothing has to cross between parts.
Inputs may be any that keep to these rules, and one draw needn't show every extreme that they name: Image k's keypoints are its first counts[k] slots. `pairs`: the two images of a pair differ.
All inputs are finite; a program needn't handle non-finite values.
Results may differ from the reference program's by a relative error of at most 0.0003.
Values may be sent and summed in bfloat16 or wider, within the bound.
No kernel may reach another device: no remote copies, remote signals or barrier semaphores. Data moves between devices by JAX's collectives and lax.ppermute only.
A program may use at most 64 MiB of HBM per device.

```python
import jax
import jax.numpy as jnp
from jax import lax

PAIRS = 4
IMAGES = 8
KP = 2048
D = 256
ITERS = 10


def draw_descriptors(key, part):
    values = 2.0 * jax.random.truncated_normal(jax.random.fold_in(key, 5), -4.0, 4.0, (IMAGES, KP, D), jnp.float32)
    return values.astype(jnp.bfloat16)


def draw_pairs(key, part):
    first_image = jax.random.randint(jax.random.fold_in(key, 1), (PAIRS,), 0, IMAGES)
    stride = jax.random.randint(jax.random.fold_in(key, 2), (PAIRS,), 1, IMAGES)
    second_image = (first_image + stride) % IMAGES
    return jnp.stack([first_image, second_image], axis=1).astype(jnp.int32)


def set_ends(entries, key, least, largest):
    spot = [jax.random.randint(jax.random.fold_in(key, axis), (), 0, length) for axis, length in enumerate(entries.shape)]
    longest = entries.shape.index(max(entries.shape))
    neighbour = spot[:longest] + [(spot[longest] + 1) % entries.shape[longest]] + spot[longest + 1:]
    return entries.at[tuple(spot)].set(least).at[tuple(neighbour)].set(largest)


def setup_inputs(seed: int = 0, part: int = 0) -> dict:
    keys = jax.random.split(jax.random.key(seed), 5)
    part_splits = jax.random.split(jax.random.fold_in(keys[4], part), 5)
    descriptors = draw_descriptors(jax.random.fold_in(jax.random.fold_in(keys[4], part), 71), part)
    counts = set_ends(jax.random.randint(part_splits[1], (IMAGES,), KP // 4, KP + 1), jax.random.fold_in(part_splits[1], 1), KP // 4, KP).astype(jnp.int32)
    pairs = draw_pairs(jax.random.fold_in(jax.random.fold_in(keys[4], part), 71), part)
    bin_score = jnp.clip(jax.random.uniform(keys[3], (1,), jnp.float32, 0.5, 2.0), 0.5, 2.0)
    return dict(descriptors=descriptors, counts=counts, pairs=pairs, bin_score=bin_score)


NEG = -1.0e30


def masked_lse(values, kept, reduce_dim):
    held = jnp.where(kept, values, NEG)
    ceiling = jnp.max(held, axis=reduce_dim, keepdims=True)
    summed = jnp.sum(jnp.where(kept, jnp.exp(held - ceiling), 0.0), axis=reduce_dim, keepdims=True)
    return jnp.squeeze(ceiling + jnp.log(summed), reduce_dim)


def reference(descriptors, counts, pairs, bin_score):
    bin_value = bin_score[0]
    row_images = descriptors[pairs[:, 0]]
    col_images = descriptors[pairs[:, 1]]
    row_counts = counts[pairs[:, 0]]
    col_counts = counts[pairs[:, 1]]

    def one_pair(operands):
        row_desc, col_desc, n_rows, n_cols = operands
        scores = jnp.dot(row_desc, col_desc.T, preferred_element_type=jnp.float32) * (D ** -0.5)
        side_line = jnp.zeros((KP, 1), jnp.float32) + bin_value
        upper = jnp.concatenate([scores, side_line], axis=1)
        bin_line = jnp.zeros((1, KP + 1), jnp.float32) + bin_value
        couplings = jnp.concatenate([upper, bin_line], axis=0)
        cell_index = jnp.arange(KP + 1, dtype=jnp.int32)
        row_kept = (cell_index < n_rows) | (cell_index == KP)
        col_kept = (cell_index < n_cols) | (cell_index == KP)
        row_count = n_rows.astype(jnp.float32)
        col_count = n_cols.astype(jnp.float32)
        log_norm = -jnp.log(row_count + col_count)
        log_mu = jnp.where(cell_index == KP, jnp.log(col_count) + log_norm, log_norm)
        log_nu = jnp.where(cell_index == KP, jnp.log(row_count) + log_norm, log_norm)
        row_pot = jnp.zeros((KP + 1,), jnp.float32)
        col_pot = jnp.zeros((KP + 1,), jnp.float32)
        for sweep_index in range(ITERS):
            row_pot = log_mu - masked_lse(couplings + col_pot[None, :], col_kept[None, :], 1)
            col_pot = log_nu - masked_lse(couplings + row_pot[:, None], row_kept[:, None], 0)
        assign = couplings + row_pot[:, None] + col_pot[None, :] - log_norm
        assign = jnp.where(row_kept[:, None] & col_kept[None, :], assign, 0.0)
        return assign[:KP, :KP], assign[:KP, KP], assign[KP, :KP]

    log_match, row_bins, col_bins = lax.map(one_pair, (row_images, col_images, row_counts, col_counts))
    return (log_match, row_bins, col_bins)
```

```python
import functools
import jax, jax.numpy as jnp
from jax import lax
from jax.sharding import PartitionSpec as P
from jax.experimental import pallas as pl
from jax.experimental.pallas import tpu as pltpu

NEG = -1e30
LANES = 128
SUB = 8
ITERS = 10
FIRST = 6

def sink_kernel(ints, bins, rd, cd, out, k, abc, mrow, bs, vs, *, kp, rb):
    wide = kp + LANES
    chunks = wide // LANES
    groups = rb // SUB
    na = ints[0]
    nb = ints[1]
    bin_v = bins[0]
    naf = na.astype(jnp.float32)
    nbf = nb.astype(jnp.float32)
    mu = 1.0 / jnp.full((SUB, LANES), naf + nbf, jnp.float32)
    mu_bin = mu[:1, :1] * nbf
    lane = lax.broadcasted_iota(jnp.int32, (1, wide), 1)
    col_ok = (lane < nb) | (lane == kp)
    nu = jnp.where(lane == kp, mu[:1, :1] * naf, mu[:1, :1])
    blocks = lax.div(na + (rb - 1), rb)
    row_in = lax.broadcasted_iota(jnp.int32, (SUB, LANES), 0)

    def piece(r0, s, c):
        return k[pl.ds(r0 + s * SUB, SUB), c * LANES:(c + 1) * LANES]

    def row_pass(n):
        r0 = pl.multiple_of(n * rb, rb)
        bc = [bs[:, c * LANES:(c + 1) * LANES] for c in range(chunks)]
        sums = []
        for s in range(groups):
            even = piece(r0, s, 0) * bc[0]
            odd = piece(r0, s, 1) * bc[1]
            for c in range(2, chunks, 2):
                even = even + piece(r0, s, c) * bc[c]
                if c + 1 < chunks:
                    odd = odd + piece(r0, s, c + 1) * bc[c + 1]
            sums.append(even + odd)
        for s in range(groups):
            total = jnp.sum(sums[s], axis=1, keepdims=True)
            scale = mu / jnp.broadcast_to(total, (SUB, LANES))
            scale = jnp.where(row_in + (r0 + s * SUB) < na, scale, 0.0)
            abc[pl.ds(r0 + s * SUB, SUB), :] = scale

    def col_pass(n, acc):
        r0 = pl.multiple_of(n * rb, rb)
        acc = list(acc)
        for s in range(groups):
            scale = abc[pl.ds(r0 + s * SUB, SUB), :]
            for c in range(chunks):
                acc[c] = acc[c] + piece(r0, s, c) * scale
        return tuple(acc)

    def window(w, carry):
        v = vs[...]
        kbin = bin_v + v
        mbin = jnp.max(kbin, axis=1, keepdims=True)
        kbin = jnp.exp(kbin - mbin)
        vbin = bin_v + v[:, kp:]

        def build(n, _):
            r0 = pl.multiple_of(n * rb, rb)
            k[pl.ds(r0, rb), :kp] = lax.dot_general(
                rd[pl.ds(r0, rb), :], cd[...], (((1,), (1,)), ((), ())), preferred_element_type=jnp.float32)
            for s in range(groups):
                rows = pl.ds(r0 + s * SUB, SUB)
                vals = [k[rows, c * LANES:(c + 1) * LANES] + v[:, c * LANES:(c + 1) * LANES]
                        for c in range(chunks - 1)]
                vals.append(jnp.broadcast_to(vbin, (SUB, LANES)))
                top = functools.reduce(jnp.maximum, vals)
                top = jnp.broadcast_to(jnp.max(top, axis=1, keepdims=True), (SUB, LANES))
                mrow[rows, :] = top
            for s in range(groups):
                rows = pl.ds(r0 + s * SUB, SUB)
                top = mrow[rows, :]
                for c in range(chunks - 1):
                    cols = slice(c * LANES, (c + 1) * LANES)
                    k[rows, cols] = jnp.exp(k[rows, cols] + v[:, cols] - top)
                k[rows, kp:] = jnp.exp(vbin - top)
            return 0
        lax.fori_loop(0, blocks, build, 0)
        bs[...] = jnp.broadcast_to(jnp.where(col_ok, 1.0, 0.0), (SUB, wide))

        def sweep(t, ubin):
            b1 = bs[:1, :]
            a_bin = mu_bin / jnp.sum(kbin * b1, axis=1, keepdims=True)
            row_pass(0)
            acc = tuple(jnp.zeros((SUB, LANES), jnp.float32) for _ in range(chunks))

            def body(n, acc):
                row_pass(n)
                return col_pass(n - 1, acc)
            acc = lax.fori_loop(1, blocks, body, acc)
            acc = col_pass(blocks - 1, acc)
            for c in range(chunks):
                cols = slice(c * LANES, (c + 1) * LANES)
                total = jnp.sum(acc[c], axis=0, keepdims=True) + a_bin * kbin[:, cols]
                bs[:, cols] = jnp.broadcast_to(jnp.where(col_ok[:, cols], nu[:, cols] / total, 0.0), (SUB, LANES))
            return jnp.log(a_bin) - mbin
        ubin = lax.fori_loop(0, jnp.where(w == 0, FIRST, ITERS - FIRST), sweep, carry)
        vs[...] = jnp.where(col_ok, v + jnp.log(jnp.where(col_ok, bs[:1, :], 1.0)), NEG)
        return ubin

    vs[...] = jnp.where(col_ok, 0.0, NEG)
    ubin = lax.fori_loop(0, 2, window, jnp.zeros((1, 1), jnp.float32))
    out[1:2, :] = jnp.where(col_ok, vs[...], 0.0)
    out[0:1, kp:] = jnp.broadcast_to(ubin, (1, LANES))
    diag = lax.broadcasted_iota(jnp.int32, (LANES, LANES), 0) == lax.broadcasted_iota(jnp.int32, (LANES, LANES), 1)
    for i in range(kp // LANES):
        rows = slice(i * LANES, (i + 1) * LANES)
        u = jnp.log(abc[rows, :]) - mrow[rows, :]
        u = jnp.sum(jnp.where(diag, u, 0.0), axis=0, keepdims=True)
        out[0:1, rows] = jnp.where(lane[:, rows] < na, u, 0.0)

def owner_kernel(ints, bins, *refs, kp, rb, ranks):
    slices = refs[:ranks]
    out, rd, cd, k, abc, mrow, bs, vs = refs[ranks:]

    @pl.when(ints[2] == 1)
    def _():
        rows = kp // ranks
        scale = jnp.bfloat16(rd.shape[1] ** (-0.5))
        for i in range(ranks):
            place = pl.ds(pl.multiple_of((ints[3] ^ i) * rows, rows), rows)
            rd[place, :] = slices[i][0] * scale
            cd[place, :] = slices[i][1]
        sink_kernel(ints, bins, rd, cd, out, k, abc, mrow, bs, vs, kp=kp, rb=rb)

    @pl.when(ints[2] == 0)
    def _():
        out[...] = jnp.zeros_like(out)


def sinkhorn(ints, bins, slices, rb=256):
    ranks = len(slices)
    _, rows, depth = slices[0].shape
    kp = rows * ranks
    wide = kp + LANES
    vmem = pl.BlockSpec(memory_space=pltpu.VMEM)
    smem = pl.BlockSpec(memory_space=pltpu.SMEM)
    return pl.pallas_call(
        functools.partial(owner_kernel, kp=kp, rb=rb, ranks=ranks),
        out_shape=jax.ShapeDtypeStruct((2, wide), jnp.float32),
        in_specs=[smem, smem] + [vmem] * ranks,
        out_specs=vmem,
        scratch_shapes=[
            pltpu.VMEM((kp, depth), jnp.bfloat16),
            pltpu.VMEM((kp, depth), jnp.bfloat16),
            pltpu.VMEM((kp, wide), jnp.float32),
            pltpu.VMEM((kp, LANES), jnp.float32),
            pltpu.VMEM((kp, LANES), jnp.float32),
            pltpu.VMEM((SUB, wide), jnp.float32),
            pltpu.VMEM((1, wide), jnp.float32),
        ],
        compiler_params=pltpu.CompilerParams(vmem_limit_bytes=40 << 20),
        name="sinkhorn",
    )(ints, bins, *slices)


def on_device(descriptors, counts, pairs, bin_score):
    local_rows, depth = descriptors.shape[1:]
    ranks = lax.axis_size("row")
    rank = lax.axis_index("row")
    pair_count = pairs.shape[0]
    all_cols = local_rows * ranks
    first = (ranks - pair_count) // 2
    row_desc = descriptors[pairs[:, 0]]
    col_desc = descriptors[pairs[:, 1]]
    n_rows = counts[pairs[:, 0]]
    n_cols = counts[pairs[:, 1]]
    all_desc = lax.all_gather(col_desc, "row", axis=1, tiled=True)
    both = jnp.stack([row_desc, col_desc], axis=1)

    def for_owner(owner):
        return lax.dynamic_index_in_dim(both, jnp.clip(owner - first, 0, pair_count - 1), 0, keepdims=False)

    slices = [for_owner(rank)]
    for i in range(1, ranks):
        links = [((first + p) ^ i, first + p) for p in range(pair_count)]
        slices.append(lax.ppermute(for_owner(rank ^ i), "row", links))
    mine = jnp.clip(rank - first, 0, pair_count - 1)
    owns = (rank >= first) & (rank < first + pair_count)
    ints = jnp.stack([n_rows[mine], n_cols[mine], owns.astype(jnp.int32), rank])
    pots = sinkhorn(ints, bin_score, slices)
    table = jnp.where((jnp.arange(pair_count) == rank - first)[:, None, None], pots[None], 0.0)
    step = 1
    while step < ranks:
        table = table + lax.ppermute(table, "row", [(r, r ^ step) for r in range(ranks)])
        step *= 2
    offset = rank * local_rows
    row_pot = lax.dynamic_slice_in_dim(table[:, 0], offset, local_rows, 1)
    row_bin = table[:, 0, all_cols]
    col_pot = table[:, 1, :all_cols]
    col_bin = table[:, 1, all_cols]
    scores = jnp.einsum("prd,pcd->prc", row_desc, all_desc, preferred_element_type=jnp.float32) * depth ** (-0.5)
    row_kept = (offset + lax.iota(jnp.int32, local_rows))[None, :] < n_rows[:, None]
    col_kept = lax.iota(jnp.int32, all_cols)[None, :] < n_cols[:, None]
    log_norm = -jnp.log(n_rows.astype(jnp.float32) + n_cols.astype(jnp.float32))
    bin_value = bin_score[0]
    both_kept = row_kept[:, :, None] & col_kept[:, None, :]
    log_match = jnp.where(
        both_kept, scores + row_pot[:, :, None] + col_pot[:, None, :] - log_norm[:, None, None], 0.0
    )
    row_bins = jnp.where(row_kept, bin_value + row_pot + col_bin[:, None] - log_norm[:, None], 0.0)
    col_bins = jnp.where(col_kept, bin_value + row_bin[:, None] + col_pot - log_norm[:, None], 0.0)
    return (log_match, row_bins, col_bins)


def solution(mesh):
    return jax.shard_map(
        on_device,
        mesh=mesh,
        in_specs=(P("pair", "row", None), P("pair"), P("pair", None), P()),
        out_specs=(P("pair", "row", None), P("pair", "row"), P("pair", None)),
        check_vma=False,
    )
```

```python
import functools

import jax
import jax.numpy as jnp
from jax import lax
from jax.experimental import pallas as pl
from jax.experimental.pallas import tpu as pltpu
from jax.sharding import PartitionSpec as P

SWEEPS = (2, 4, 4)
SPREAD = 64.0
NEG = -1e30
LANES = 128
SUB = 8
TILE = 256
TALL = 512
STEPS = 4
SINK_FLOPS = 100_000_000


def spread(row):
    diag = lax.broadcasted_iota(jnp.int32, (LANES, LANES), 0) == lax.broadcasted_iota(jnp.int32, (LANES, LANES), 1)
    return jnp.sum(jnp.where(diag, row, 0.0), axis=1, keepdims=True)


def gather_row(tall):
    diag = lax.broadcasted_iota(jnp.int32, (LANES, LANES), 0) == lax.broadcasted_iota(jnp.int32, (LANES, LANES), 1)
    return jnp.sum(jnp.where(diag, tall, 0.0), axis=0, keepdims=True)


def lanes(c):
    return slice(c * LANES, (c + 1) * LANES)


class Pair:
    def __init__(self, na, nb, bin_v, kp, rb, steps):
        self.na, self.nb, self.bin_v, self.kp, self.rb = na, nb, bin_v, kp, rb
        self.wide = kp + LANES
        self.used = steps * (kp // STEPS)
        self.cols = [lanes(c) for c in range(self.used // LANES)] + [slice(kp, self.wide)]
        self.groups = rb // SUB
        self.per = TALL // rb
        lane = lax.broadcasted_iota(jnp.int32, (1, self.wide), 1)
        self.lane = lane
        self.col_ok = (lane < nb) | (lane == kp)
        naf = na.astype(jnp.float32)
        nbf = nb.astype(jnp.float32)
        self.mu = 1.0 / jnp.full((SUB, LANES), naf + nbf, jnp.float32)
        self.mu_bin = self.mu[:1, :1] * nbf
        self.nu = jnp.where(lane == kp, self.mu[:1, :1] * naf, self.mu[:1, :1])
        self.blocks = lax.div(na + (rb - 1), rb)
        self.talls = lax.div(na + (TALL - 1), TALL)

    def dot(self, rd, cd, i, j):
        rows = pl.ds(pl.multiple_of(i * TALL, TALL), TALL)
        return lax.dot_general(
            rd[rows, :], cd[j * TILE : (j + 1) * TILE, :], (((1,), (1,)), ((), ())),
            preferred_element_type=jnp.float32,
        )

    def bin_lane(self, v):
        return jnp.where(self.lane[:, self.kp :] == self.kp, self.bin_v + v[:, self.kp :], NEG)

    def ones(self, bs):
        bs[...] = jnp.broadcast_to(jnp.where(self.col_ok, 1.0, 0.0), (SUB, self.wide))

    def build(self, rd, cd, k, mrow, bs, gap):
        rb, vbin = self.rb, self.bin_lane(jnp.zeros((1, self.wide), jnp.float32))

        def scores(i, low):
            for j in range(self.used // TILE):
                s = self.dot(rd, cd, i, j)
                for h in range(self.per):
                    n = i * self.per + h
                    part = s[h * rb : (h + 1) * rb]
                    k[n, :, j * TILE : (j + 1) * TILE] = part
                    top = jnp.maximum(part[:, :LANES], part[:, LANES:])
                    mrow[n] = top if j == 0 else jnp.maximum(mrow[n], top)
                    least = jnp.minimum(part[:, :LANES], part[:, LANES:])
                    low = jnp.minimum(low, jnp.min(least.reshape(self.groups, SUB, LANES), axis=0))
            return low

        low = lax.fori_loop(0, self.talls, scores, jnp.zeros((SUB, LANES), jnp.float32))

        def scale_down(n, high):
            for s in range(self.groups):
                rows = slice(s * SUB, (s + 1) * SUB)
                top = jnp.max(jnp.maximum(mrow[n, rows, :], vbin), axis=1, keepdims=True)
                top = jnp.broadcast_to(top, (SUB, LANES))
                mrow[n, rows, :] = top
                high = jnp.maximum(high, top)
            for s in range(self.groups):
                rows = slice(s * SUB, (s + 1) * SUB)
                top = mrow[n, rows, :]
                for c in self.cols[:-1]:
                    k[n, rows, c] = jnp.exp(k[n, rows, c] - top)
                k[n, rows, self.kp :] = jnp.exp(vbin - top)
            return high

        high = lax.fori_loop(0, self.blocks, scale_down, jnp.zeros((SUB, LANES), jnp.float32))
        gap[0] = jnp.max(high) - jnp.min(low)
        self.ones(bs)

    def rebuild(self, rd, cd, k, scale, mrow, bs, vs):
        rb = self.rb
        log_mu = jnp.log(self.mu[:1])
        v = jnp.where(self.col_ok, jnp.log(jnp.where(self.col_ok, bs[:1, :], 1.0)), NEG)
        vs[...] = v
        vbin = self.bin_lane(v)

        def block(i, _):
            for g in range(self.per):
                n = i * self.per + g
                row = lax.broadcasted_iota(jnp.int32, (rb, LANES), 0) + n * rb
                a = jnp.where(row < self.na, scale[n], 1.0)
                mrow[n] = jnp.where(row < self.na, mrow[n] + log_mu - jnp.log(a), -NEG)
            for j in range(self.used // TILE):
                s = self.dot(rd, cd, i, j)
                for g in range(self.per):
                    n = i * self.per + g
                    top = mrow[n]
                    for h in range(TILE // LANES):
                        c = lanes(j * (TILE // LANES) + h)
                        k[n, :, c] = jnp.exp((s[g * rb : (g + 1) * rb, lanes(h)] + v[:, c]) - top)
            for g in range(self.per):
                k[i * self.per + g, :, self.kp :] = jnp.exp(vbin - mrow[i * self.per + g])
            return 0

        lax.fori_loop(0, self.talls, block, 0)
        self.ones(bs)

    def sweep(self, sweeps, k, scale, bs, v):
        na, rb, groups, cols = self.na, self.rb, self.groups, self.cols
        sub = lax.broadcasted_iota(jnp.int32, (SUB, LANES), 0)
        kbin = jnp.where(self.col_ok, self.bin_v + v, NEG)
        mbin = jnp.max(kbin, axis=1, keepdims=True)
        kbin = jnp.exp(kbin - mbin)

        def row_pass(n):
            left = na - n * rb - sub
            b = [bs[:, c] for c in cols]
            sums = []
            for s in range(groups):
                rows = slice(s * SUB, (s + 1) * SUB)
                parts = [None, None]
                for i, c in enumerate(cols):
                    term = k[n, rows, c] * b[i]
                    parts[i % 2] = term if parts[i % 2] is None else parts[i % 2] + term
                sums.append(parts[0] + parts[1])
            for s in range(groups):
                total = jnp.broadcast_to(jnp.sum(sums[s], axis=1, keepdims=True), (SUB, LANES))
                scale[n, s * SUB : (s + 1) * SUB, :] = jnp.where(left > s * SUB, self.mu / total, 0.0)

        def col_pass(n, acc):
            acc = list(acc)
            for s in range(groups):
                rows = slice(s * SUB, (s + 1) * SUB)
                a = scale[n, rows, :]
                for i, c in enumerate(cols):
                    acc[i] = acc[i] + k[n, rows, c] * a
            return tuple(acc)

        def once(_, ubin):
            a_bin = self.mu_bin / jnp.sum(kbin * bs[:1, :], axis=1, keepdims=True)
            row_pass(0)
            acc = tuple(jnp.zeros((SUB, LANES), jnp.float32) for _ in cols)

            def body(n, acc):
                row_pass(n + 1)
                return col_pass(n, acc)

            acc = col_pass(self.blocks - 1, lax.fori_loop(0, self.blocks - 1, body, acc))
            for i, c in enumerate(cols):
                total = jnp.sum(acc[i], axis=0, keepdims=True) + a_bin * kbin[:, c]
                b = jnp.where(self.col_ok[:, c], self.nu[:, c] / total, 0.0)
                bs[:, c] = jnp.broadcast_to(b, (SUB, LANES))
            return jnp.log(a_bin) - mbin

        return lax.fori_loop(0, sweeps, once, jnp.zeros((1, 1), jnp.float32))

    def finish(self, ubin, scale, mrow, bs, v, out):
        kp, rb = self.kp, self.rb
        out[1:2, :] = jnp.where(self.col_ok, v + jnp.log(jnp.where(self.col_ok, bs[:1, :], 1.0)), 0.0)
        out[0:1, kp:] = jnp.broadcast_to(ubin, (1, LANES))
        for i in range(kp // LANES):
            n, rows = i * LANES // rb, slice(i * LANES % rb, i * LANES % rb + LANES)
            u = gather_row(jnp.log(scale[n, rows, :]) - mrow[n, rows, :])
            out[0:1, lanes(i)] = jnp.where(self.lane[:, lanes(i)] < self.na, u, 0.0)


def load(slices, stage, sems, rd, cd, rank, nb):
    ranks = len(slices)
    rows = rd.shape[0] // ranks
    copies = [pltpu.make_async_copy(slices[i], stage.at[i], sems.at[i]) for i in range(ranks)]
    for copy in copies:
        copy.start()
    factor = jnp.bfloat16(rd.shape[1] ** (-0.5))
    for i in range(ranks):
        copies[i].wait()
        start = pl.multiple_of((rank ^ i) * rows, rows)
        rd[pl.ds(start, rows), :] = stage[i, 0] * factor
        inside = lax.broadcasted_iota(jnp.int32, (rows, 1), 0) + start < nb
        cd[pl.ds(start, rows), :] = jnp.where(inside, stage[i, 1], 0).astype(jnp.bfloat16)


def for_pair(place, counts, pairs, bins, kp, rb, ranks, run, idle=None):
    rank = place[0]
    pair_count = pairs.shape[0] // 2
    pair = rank - (ranks - pair_count) // 2
    owns = (pair >= 0) & (pair < pair_count)
    mine = jnp.clip(pair, 0, pair_count - 1)
    na = counts[pairs[2 * mine]]
    nb = counts[pairs[2 * mine + 1]]
    quarter = kp // STEPS
    for steps in range(1, STEPS + 1):
        @pl.when(owns & (lax.div(nb + (quarter - 1), quarter) == steps))
        def _():
            run(rank, Pair(na, nb, bins[0], kp, rb, steps))
    if idle is not None:
        @pl.when(~owns)
        def _():
            idle()


def first_kernel(place, counts, pairs, bins, *refs, kp, rb, ranks, sweeps):
    slices = refs[:ranks]
    k, scale, mrow, bs, gap, stage, sems, rd, cd = refs[ranks:]

    def run(rank, pair):
        load(slices, stage, sems, rd, cd, rank, pair.nb)
        pair.build(rd, cd, k, mrow, bs, gap)
        pair.sweep(sweeps, k, scale, bs, jnp.zeros((1, pair.wide), jnp.float32))

    def idle():
        gap[0] = 0.0

    for_pair(place, counts, pairs, bins, kp, rb, ranks, run, idle)


def middle_kernel(place, counts, pairs, bins, k, scale_in, bs_in, scale, bs, *, kp, rb, ranks, sweeps):
    def run(rank, pair):
        pair.sweep(sweeps, k, scale, bs, jnp.zeros((1, pair.wide), jnp.float32))

    for_pair(place, counts, pairs, bins, kp, rb, ranks, run)


def last_kernel(place, counts, pairs, bins, gap, *refs, kp, rb, ranks, sweeps):
    slices = refs[:ranks]
    k, scale, mrow, bs, out, stage, sems, rd, cd, vs = refs[ranks + 4 :]

    def run(rank, pair):
        vs[...] = jnp.zeros_like(vs)

        @pl.when(gap[0] > SPREAD)
        def _():
            load(slices, stage, sems, rd, cd, rank, pair.nb)
            pair.rebuild(rd, cd, k, scale, mrow, bs, vs)

        v = vs[...]
        pair.finish(pair.sweep(sweeps, k, scale, bs, v), scale, mrow, bs, v, out)

    def idle():
        out[...] = jnp.zeros_like(out)

    for_pair(place, counts, pairs, bins, kp, rb, ranks, run, idle)


def stages(scalars, slices, rb=256):
    ranks = len(slices)
    _, rows, depth = slices[0].shape
    kp = rows * ranks
    wide = kp + LANES
    vmem = pl.BlockSpec(memory_space=pltpu.VMEM)
    smem = pl.BlockSpec(memory_space=pltpu.SMEM)
    hbm = pl.BlockSpec(memory_space=pltpu.HBM)
    matrix = pltpu.VMEM((kp // rb, rb, wide), jnp.float32)
    tall = pltpu.VMEM((kp // rb, rb, LANES), jnp.float32)
    line = pltpu.VMEM((SUB, wide), jnp.float32)
    inputs = [
        pltpu.VMEM((ranks, 2, rows, depth), jnp.bfloat16),
        pltpu.SemaphoreType.DMA((ranks,)),
        pltpu.VMEM((kp, depth), jnp.bfloat16),
        pltpu.VMEM((kp, depth), jnp.bfloat16),
    ]
    kernel = functools.partial(functools.partial, kp=kp, rb=rb, ranks=ranks)
    params = pltpu.CompilerParams(vmem_limit_bytes=12 << 20)
    cost = pl.CostEstimate(flops=SINK_FLOPS, bytes_accessed=4 * kp * depth, transcendentals=0)

    def first():
        return pl.pallas_call(
            kernel(first_kernel, sweeps=SWEEPS[0]),
            out_shape=(matrix, tall, tall, line, jax.ShapeDtypeStruct((1,), jnp.float32)),
            in_specs=[smem] * 4 + [hbm] * ranks,
            out_specs=(vmem, vmem, vmem, vmem, smem),
            scratch_shapes=inputs,
            compiler_params=params,
            cost_estimate=cost,
            name="sinkhorn_first",
        )(*scalars, *slices)

    def middle(state):
        k, scale, mrow, bs, gap = state
        scale, bs = pl.pallas_call(
            kernel(middle_kernel, sweeps=SWEEPS[1]),
            out_shape=(tall, line),
            in_specs=[smem] * 4 + [vmem] * 3,
            out_specs=(vmem, vmem),
            input_output_aliases={5: 0, 6: 1},
            compiler_params=params,
            cost_estimate=cost,
            name="sinkhorn_middle",
        )(*scalars, k, scale, bs)
        return k, scale, mrow, bs, gap

    def last(state):
        k, scale, mrow, bs, gap = state
        return pl.pallas_call(
            kernel(last_kernel, sweeps=SWEEPS[2]),
            out_shape=(matrix, tall, tall, line, jax.ShapeDtypeStruct((2, wide), jnp.float32)),
            in_specs=[smem] * 5 + [hbm] * ranks + [vmem] * 4,
            out_specs=(vmem,) * 5,
            input_output_aliases={5 + ranks + i: i for i in range(4)},
            scratch_shapes=inputs + [pltpu.VMEM((1, wide), jnp.float32)],
            compiler_params=params,
            cost_estimate=cost,
            name="sinkhorn_last",
        )(*scalars, gap, *slices, k, scale, mrow, bs)[4]

    return first, middle, last


def hop_of(i):
    return (i + 1) // 2 if i % 2 == 0 else -((i + 1) // 2)


def ring_at(place, ranks):
    return jnp.where(place < ranks // 2, 2 * place, 2 * (ranks - 1 - place) + 1)


def match_kernel(place, counts, pairs, bins, row_desc, *refs, ranks, rows, pair_count):
    tables = refs[: ranks // 2]
    chunks = refs[ranks // 2 : ranks // 2 + ranks + 1]
    log_match, row_bins, col_bins, table = refs[ranks // 2 + ranks + 1 :]
    p = pl.program_id(0)
    kp = rows * ranks
    rank = place[0]
    na = counts[pairs[2 * p]]
    nb = counts[pairs[2 * p + 1]]
    away = (((ranks - pair_count) // 2 + p) ^ rank) // 2
    for i in range(ranks // 2):
        @pl.when(away == i)
        def _():
            table[0] = tables[i][lax.rem(p, 2)]
    at = jnp.where(lax.rem(rank, 2) == 0, rank // 2, ranks - 1 - rank // 2)
    offset = pl.multiple_of(rank * rows, rows)
    log_norm = -jnp.log(jnp.full((1, 1), na + nb, jnp.int32).astype(jnp.float32))
    bin_v = bins[0]
    u = table[0, 0:1, pl.ds(offset, rows)]
    u_bin = table[0, 0:1, kp : kp + 1]
    v_bin = table[0, 1:2, kp : kp + 1]
    lane = lax.broadcasted_iota(jnp.int32, (1, kp), 1)
    row_ok = lane[:, :rows] + offset < na
    row_bins[pl.ds(p, 1), :] = jnp.where(row_ok, bin_v + u + v_bin - log_norm, 0.0)
    col_bins[pl.ds(p, 1), :] = jnp.where(lane < nb, bin_v + u_bin + table[0, 1:2, :kp] - log_norm, 0.0)
    u_tall = [spread(u[:, lanes(i)]) for i in range(rows // LANES)]
    u_tall = u_tall[0] if len(u_tall) == 1 else jnp.concatenate(u_tall, axis=0)
    inside = lax.broadcasted_iota(jnp.int32, (rows, 1), 0) + offset < na
    factor = jnp.bfloat16(row_desc.shape[2] ** (-0.5))
    mine = row_desc[0] * factor
    for i in range(ranks):
        start = pl.multiple_of(ring_at(lax.rem(at + ranks + hop_of(i), ranks), ranks) * rows, rows)
        desc = chunks[i][0] if i + 1 < ranks else jnp.where(p < pair_count // 2, chunks[i][0], chunks[i + 1][0])
        s = lax.dot_general(mine, desc, (((1,), (1,)), ((), ())), preferred_element_type=jnp.float32)
        v = table[0, 1:2, pl.ds(start, rows)] - log_norm
        ok = inside & (lane[:, :rows] + start < nb)
        log_match[0, :, pl.ds(start, rows)] = jnp.where(ok, s + u_tall + v, 0.0)


def finish(scalars, row_desc, tables, chunks):
    pair_count, rows, depth = row_desc.shape
    ranks = len(chunks) - 1
    kp = rows * ranks
    half = pair_count // 2
    smem = pl.BlockSpec(memory_space=pltpu.SMEM)
    each = pl.BlockSpec((1, rows, depth), lambda p: (p, 0, 0))
    specs = [each] * (ranks - 1) + [
        pl.BlockSpec((1, rows, depth), lambda p: (jnp.minimum(p, half - 1), 0, 0)),
        pl.BlockSpec((1, rows, depth), lambda p: (jnp.maximum(p - half, 0), 0, 0)),
    ]
    return pl.pallas_call(
        functools.partial(match_kernel, ranks=ranks, rows=rows, pair_count=pair_count),
        grid=(pair_count,),
        out_shape=(
            jax.ShapeDtypeStruct((pair_count, rows, kp), jnp.float32),
            jax.ShapeDtypeStruct((pair_count, rows), jnp.float32),
            jax.ShapeDtypeStruct((pair_count, kp), jnp.float32),
        ),
        in_specs=[smem] * 4 + [each] + [pl.BlockSpec(x.shape, lambda p: (0, 0, 0)) for x in tables] + specs,
        out_specs=(
            pl.BlockSpec((1, rows, kp), lambda p: (p, 0, 0)),
            pl.BlockSpec((pair_count, rows), lambda p: (0, 0)),
            pl.BlockSpec((pair_count, kp), lambda p: (0, 0)),
        ),
        scratch_shapes=[pltpu.VMEM((1,) + tables[0].shape[1:], jnp.float32)],
        compiler_params=pltpu.CompilerParams(vmem_limit_bytes=60 << 20),
        name="match",
    )(*scalars, row_desc, *tables, *chunks)


def completed(links, ranks):
    sources = [r for r in range(ranks) if r not in [a for a, _ in links]]
    targets = [r for r in range(ranks) if r not in [b for _, b in links]]
    return links + list(zip(sources, targets))


def on_device(descriptors, counts, pairs, bin_score):
    local_rows, depth = descriptors.shape[1:]
    ranks = lax.axis_size("row")
    rank = lax.axis_index("row")
    pair_count = pairs.shape[0]
    first = (ranks - pair_count) // 2
    row_desc = descriptors[pairs[:, 0]]
    col_desc = descriptors[pairs[:, 1]]
    both = jnp.stack([row_desc, col_desc], axis=1)

    def for_owner(owner):
        return lax.dynamic_index_in_dim(both, jnp.clip(owner - first, 0, pair_count - 1), 0, keepdims=False)

    messages = [for_owner(rank ^ i) for i in range(ranks)]
    flat, col_desc, messages = lax.optimization_barrier((pairs.reshape(-1), col_desc, messages))
    scalars = (rank[None], counts, flat, bin_score)
    slices = [messages[0]]
    for i in range(1, ranks):
        links = completed([((first + p) ^ i, first + p) for p in range(pair_count)], ranks)
        slices.append(lax.ppermute(messages[i], "row", links))
    ring = list(range(0, ranks, 2)) + list(range(1, ranks, 2))[::-1]
    ahead = [(ring[i], ring[(i + 1) % ranks]) for i in range(ranks)]
    behind = [(b, a) for a, b in ahead]
    chunks = [col_desc]

    def hop(step, fore, back):
        if step == ranks // 2:
            half = pair_count // 2
            fore, back = fore[:half], back[half:]
        fore = lax.ppermute(fore, "row", ahead)
        back = lax.ppermute(back, "row", behind)
        chunks.extend([fore, back])
        return fore, back

    slices, col_desc = lax.optimization_barrier((slices, col_desc))
    first_stage, middle_stage, last_stage = stages(scalars, slices)
    fore, back = hop(1, col_desc, col_desc)
    state = first_stage()
    bs, fore, back = lax.optimization_barrier((state[3], fore, back))
    fore, back = hop(2, fore, back)
    state = middle_stage((*state[:3], bs, state[4]))
    bs, fore, back = lax.optimization_barrier((state[3], fore, back))
    fore, back = hop(3, fore, back)
    pots = last_stage((*state[:3], bs, state[4]))
    pots, fore, back = lax.optimization_barrier((pots, fore, back))
    for step in range(4, ranks // 2 + 1):
        fore, back = hop(step, fore, back)
    other = lax.ppermute(pots, "row", [(r, r ^ 1) for r in range(ranks)])
    odd = lax.rem(rank, 2) == 1
    table = jnp.stack([jnp.where(odd, other, pots), jnp.where(odd, pots, other)])
    tables = [table]
    for i in range(2, ranks, 2):
        links = completed([(first + p, (first + p) ^ i) for p in range(pair_count)], ranks)
        tables.append(lax.ppermute(table, "row", links))
    return finish(scalars, row_desc, tables, chunks)


def solution(mesh):
    return jax.shard_map(
        on_device,
        mesh=mesh,
        in_specs=(P("pair", "row", None), P("pair"), P("pair", None), P()),
        out_specs=(P("pair", "row", None), P("pair", "row"), P("pair", None)),
        check_vma=False,
    )
```

```python
import functools

import jax
import jax.numpy as jnp
from jax import lax
from jax.experimental import pallas as pl
from jax.experimental.pallas import tpu as pltpu
from jax.sharding import PartitionSpec as P

SWEEPS = (2, 4, 4)
SPREAD = 64.0
NEG = -1e30
LANES = 128
SUB = 8
TILE = 256
TALL = 512
STEPS = 4
SINK_FLOPS = 100_000_000


def spread(row):
    diag = lax.broadcasted_iota(jnp.int32, (LANES, LANES), 0) == lax.broadcasted_iota(jnp.int32, (LANES, LANES), 1)
    return jnp.sum(jnp.where(diag, row, 0.0), axis=1, keepdims=True)


def gather_row(tall):
    diag = lax.broadcasted_iota(jnp.int32, (LANES, LANES), 0) == lax.broadcasted_iota(jnp.int32, (LANES, LANES), 1)
    return jnp.sum(jnp.where(diag, tall, 0.0), axis=0, keepdims=True)


def lanes(c):
    return slice(c * LANES, (c + 1) * LANES)


class Pair:
    def __init__(self, na, nb, bin_v, kp, rb, steps):
        self.na, self.nb, self.bin_v, self.kp, self.rb = na, nb, bin_v, kp, rb
        self.wide = kp + LANES
        self.used = steps * (kp // STEPS)
        self.cols = [lanes(c) for c in range(self.used // LANES)] + [slice(kp, self.wide)]
        self.groups = rb // SUB
        self.per = TALL // rb
        lane = lax.broadcasted_iota(jnp.int32, (1, self.wide), 1)
        self.lane = lane
        self.col_ok = (lane < nb) | (lane == kp)
        naf = na.astype(jnp.float32)
        nbf = nb.astype(jnp.float32)
        self.mu = 1.0 / jnp.full((SUB, LANES), naf + nbf, jnp.float32)
        self.mu_bin = self.mu[:1, :1] * nbf
        self.nu = jnp.where(lane == kp, self.mu[:1, :1] * naf, self.mu[:1, :1])
        self.blocks = lax.div(na + (rb - 1), rb)
        self.talls = lax.div(na + (TALL - 1), TALL)

    def dot(self, rd, cd, i, j):
        rows = pl.ds(pl.multiple_of(i * TALL, TALL), TALL)
        return lax.dot_general(
            rd[rows, :], cd[j * TILE : (j + 1) * TILE, :], (((1,), (1,)), ((), ())),
            preferred_element_type=jnp.float32,
        )

    def bin_lane(self, v):
        return jnp.where(self.lane[:, self.kp :] == self.kp, self.bin_v + v[:, self.kp :], NEG)

    def ones(self, bs):
        bs[...] = jnp.broadcast_to(jnp.where(self.col_ok, 1.0, 0.0), (SUB, self.wide))

    def build(self, rd, cd, k, mrow, bs, gap):
        rb, vbin = self.rb, self.bin_lane(jnp.zeros((1, self.wide), jnp.float32))

        def scores(i, low):
            for j in range(self.used // TILE):
                s = self.dot(rd, cd, i, j)
                for h in range(self.per):
                    n = i * self.per + h
                    part = s[h * rb : (h + 1) * rb]
                    k[n, :, j * TILE : (j + 1) * TILE] = part
                    top = jnp.maximum(part[:, :LANES], part[:, LANES:])
                    mrow[n] = top if j == 0 else jnp.maximum(mrow[n], top)
                    least = jnp.minimum(part[:, :LANES], part[:, LANES:])
                    low = jnp.minimum(low, jnp.min(least.reshape(self.groups, SUB, LANES), axis=0))
            return low

        low = lax.fori_loop(0, self.talls, scores, jnp.zeros((SUB, LANES), jnp.float32))

        def scale_down(n, high):
            for s in range(self.groups):
                rows = slice(s * SUB, (s + 1) * SUB)
                top = jnp.max(jnp.maximum(mrow[n, rows, :], vbin), axis=1, keepdims=True)
                top = jnp.broadcast_to(top, (SUB, LANES))
                mrow[n, rows, :] = top
                high = jnp.maximum(high, top)
            for s in range(self.groups):
                rows = slice(s * SUB, (s + 1) * SUB)
                top = mrow[n, rows, :]
                for c in self.cols[:-1]:
                    k[n, rows, c] = jnp.exp(k[n, rows, c] - top)
                k[n, rows, self.kp :] = jnp.exp(vbin - top)
            return high

        high = lax.fori_loop(0, self.blocks, scale_down, jnp.zeros((SUB, LANES), jnp.float32))
        gap[0] = jnp.max(high) - jnp.min(low)
        self.ones(bs)

    def rebuild(self, rd, cd, k, scale, mrow, bs, vs):
        rb = self.rb
        log_mu = jnp.log(self.mu[:1])
        v = jnp.where(self.col_ok, jnp.log(jnp.where(self.col_ok, bs[:1, :], 1.0)), NEG)
        vs[...] = v
        vbin = self.bin_lane(v)

        def block(i, _):
            for g in range(self.per):
                n = i * self.per + g
                row = lax.broadcasted_iota(jnp.int32, (rb, LANES), 0) + n * rb
                a = jnp.where(row < self.na, scale[n], 1.0)
                mrow[n] = jnp.where(row < self.na, mrow[n] + log_mu - jnp.log(a), -NEG)
            for j in range(self.used // TILE):
                s = self.dot(rd, cd, i, j)
                for g in range(self.per):
                    n = i * self.per + g
                    top = mrow[n]
                    for h in range(TILE // LANES):
                        c = lanes(j * (TILE // LANES) + h)
                        k[n, :, c] = jnp.exp((s[g * rb : (g + 1) * rb, lanes(h)] + v[:, c]) - top)
            for g in range(self.per):
                k[i * self.per + g, :, self.kp :] = jnp.exp(vbin - mrow[i * self.per + g])
            return 0

        lax.fori_loop(0, self.talls, block, 0)
        self.ones(bs)

    def sweep(self, sweeps, k, scale, bs, v):
        na, rb, groups, cols = self.na, self.rb, self.groups, self.cols
        sub = lax.broadcasted_iota(jnp.int32, (SUB, LANES), 0)
        kbin = jnp.where(self.col_ok, self.bin_v + v, NEG)
        mbin = jnp.max(kbin, axis=1, keepdims=True)
        kbin = jnp.exp(kbin - mbin)

        def row_pass(n):
            left = na - n * rb - sub
            b = [bs[:, c] for c in cols]
            sums = []
            for s in range(groups):
                rows = slice(s * SUB, (s + 1) * SUB)
                parts = [None, None]
                for i, c in enumerate(cols):
                    term = k[n, rows, c] * b[i]
                    parts[i % 2] = term if parts[i % 2] is None else parts[i % 2] + term
                sums.append(parts[0] + parts[1])
            for s in range(groups):
                total = jnp.broadcast_to(jnp.sum(sums[s], axis=1, keepdims=True), (SUB, LANES))
                scale[n, s * SUB : (s + 1) * SUB, :] = jnp.where(left > s * SUB, self.mu / total, 0.0)

        def col_pass(n, acc):
            acc = list(acc)
            for s in range(groups):
                rows = slice(s * SUB, (s + 1) * SUB)
                a = scale[n, rows, :]
                for i, c in enumerate(cols):
                    acc[i] = acc[i] + k[n, rows, c] * a
            return tuple(acc)

        def once(_, ubin):
            a_bin = self.mu_bin / jnp.sum(kbin * bs[:1, :], axis=1, keepdims=True)
            row_pass(0)
            acc = tuple(jnp.zeros((SUB, LANES), jnp.float32) for _ in cols)

            def body(n, acc):
                row_pass(n + 1)
                return col_pass(n, acc)

            acc = col_pass(self.blocks - 1, lax.fori_loop(0, self.blocks - 1, body, acc))
            for i, c in enumerate(cols):
                total = jnp.sum(acc[i], axis=0, keepdims=True) + a_bin * kbin[:, c]
                b = jnp.where(self.col_ok[:, c], self.nu[:, c] / total, 0.0)
                bs[:, c] = jnp.broadcast_to(b, (SUB, LANES))
            return jnp.log(a_bin) - mbin

        return lax.fori_loop(0, sweeps, once, jnp.zeros((1, 1), jnp.float32))

    def finish(self, ubin, scale, mrow, bs, v, out):
        kp, rb = self.kp, self.rb
        out[1:2, :] = jnp.where(self.col_ok, v + jnp.log(jnp.where(self.col_ok, bs[:1, :], 1.0)), 0.0)
        out[0:1, kp:] = jnp.broadcast_to(ubin, (1, LANES))
        for i in range(kp // LANES):
            n, rows = i * LANES // rb, slice(i * LANES % rb, i * LANES % rb + LANES)
            u = gather_row(jnp.log(scale[n, rows, :]) - mrow[n, rows, :])
            out[0:1, lanes(i)] = jnp.where(self.lane[:, lanes(i)] < self.na, u, 0.0)


def load(slices, stage, sems, rd, cd, rank, nb):
    ranks = len(slices)
    rows = rd.shape[0] // ranks
    copies = [pltpu.make_async_copy(slices[i], stage.at[i], sems.at[i]) for i in range(ranks)]
    for copy in copies:
        copy.start()
    factor = jnp.bfloat16(rd.shape[1] ** (-0.5))
    for i in range(ranks):
        copies[i].wait()
        start = pl.multiple_of((rank ^ i) * rows, rows)
        rd[pl.ds(start, rows), :] = stage[i, 0] * factor
        inside = lax.broadcasted_iota(jnp.int32, (rows, 1), 0) + start < nb
        cd[pl.ds(start, rows), :] = jnp.where(inside, stage[i, 1], 0).astype(jnp.bfloat16)


def for_pair(place, counts, pairs, bins, kp, rb, ranks, run, idle=None):
    rank = place[0]
    pair_count = pairs.shape[0] // 2
    pair = rank - (ranks - pair_count) // 2
    owns = (pair >= 0) & (pair < pair_count)
    mine = jnp.clip(pair, 0, pair_count - 1)
    na = counts[pairs[2 * mine]]
    nb = counts[pairs[2 * mine + 1]]
    quarter = kp // STEPS
    for steps in range(1, STEPS + 1):
        @pl.when(owns & (lax.div(nb + (quarter - 1), quarter) == steps))
        def _():
            run(rank, Pair(na, nb, bins[0], kp, rb, steps))
    if idle is not None:
        @pl.when(~owns)
        def _():
            idle()


def first_kernel(place, counts, pairs, bins, *refs, kp, rb, ranks, sweeps):
    slices = refs[:ranks]
    k, scale, mrow, bs, gap, stage, sems, rd, cd = refs[ranks:]

    def run(rank, pair):
        load(slices, stage, sems, rd, cd, rank, pair.nb)
        pair.build(rd, cd, k, mrow, bs, gap)
        pair.sweep(sweeps, k, scale, bs, jnp.zeros((1, pair.wide), jnp.float32))

    def idle():
        gap[0] = 0.0

    for_pair(place, counts, pairs, bins, kp, rb, ranks, run, idle)


def middle_kernel(place, counts, pairs, bins, k, scale_in, bs_in, scale, bs, *, kp, rb, ranks, sweeps):
    def run(rank, pair):
        pair.sweep(sweeps, k, scale, bs, jnp.zeros((1, pair.wide), jnp.float32))

    for_pair(place, counts, pairs, bins, kp, rb, ranks, run)


def last_kernel(place, counts, pairs, bins, gap, *refs, kp, rb, ranks, sweeps):
    slices = refs[:ranks]
    k, scale, mrow, bs, out, stage, sems, rd, cd, vs = refs[ranks + 4 :]

    def run(rank, pair):
        vs[...] = jnp.zeros_like(vs)

        @pl.when(gap[0] > SPREAD)
        def _():
            load(slices, stage, sems, rd, cd, rank, pair.nb)
            pair.rebuild(rd, cd, k, scale, mrow, bs, vs)

        v = vs[...]
        pair.finish(pair.sweep(sweeps, k, scale, bs, v), scale, mrow, bs, v, out)

    def idle():
        out[...] = jnp.zeros_like(out)

    for_pair(place, counts, pairs, bins, kp, rb, ranks, run, idle)


def stages(scalars, slices, rb=256):
    ranks = len(slices)
    _, rows, depth = slices[0].shape
    kp = rows * ranks
    wide = kp + LANES
    vmem = pl.BlockSpec(memory_space=pltpu.VMEM)
    smem = pl.BlockSpec(memory_space=pltpu.SMEM)
    hbm = pl.BlockSpec(memory_space=pltpu.HBM)
    matrix = pltpu.VMEM((kp // rb, rb, wide), jnp.float32)
    tall = pltpu.VMEM((kp // rb, rb, LANES), jnp.float32)
    line = pltpu.VMEM((SUB, wide), jnp.float32)
    inputs = [
        pltpu.VMEM((ranks, 2, rows, depth), jnp.bfloat16),
        pltpu.SemaphoreType.DMA((ranks,)),
        pltpu.VMEM((kp, depth), jnp.bfloat16),
        pltpu.VMEM((kp, depth), jnp.bfloat16),
    ]
    kernel = functools.partial(functools.partial, kp=kp, rb=rb, ranks=ranks)
    params = pltpu.CompilerParams(vmem_limit_bytes=12 << 20)
    cost = pl.CostEstimate(flops=SINK_FLOPS, bytes_accessed=4 * kp * depth, transcendentals=0)

    def first():
        return pl.pallas_call(
            kernel(first_kernel, sweeps=SWEEPS[0]),
            out_shape=(matrix, tall, tall, line, jax.ShapeDtypeStruct((1,), jnp.float32)),
            in_specs=[smem] * 4 + [hbm] * ranks,
            out_specs=(vmem, vmem, vmem, vmem, smem),
            scratch_shapes=inputs,
            compiler_params=params,
            cost_estimate=cost,
            name="sinkhorn_first",
        )(*scalars, *slices)

    def middle(state):
        k, scale, mrow, bs, gap = state
        scale, bs = pl.pallas_call(
            kernel(middle_kernel, sweeps=SWEEPS[1]),
            out_shape=(tall, line),
            in_specs=[smem] * 4 + [vmem] * 3,
            out_specs=(vmem, vmem),
            input_output_aliases={5: 0, 6: 1},
            compiler_params=params,
            cost_estimate=cost,
            name="sinkhorn_middle",
        )(*scalars, k, scale, bs)
        return k, scale, mrow, bs, gap

    def last(state):
        k, scale, mrow, bs, gap = state
        return pl.pallas_call(
            kernel(last_kernel, sweeps=SWEEPS[2]),
            out_shape=(matrix, tall, tall, line, jax.ShapeDtypeStruct((2, wide), jnp.float32)),
            in_specs=[smem] * 5 + [hbm] * ranks + [vmem] * 4,
            out_specs=(vmem,) * 5,
            input_output_aliases={5 + ranks + i: i for i in range(4)},
            scratch_shapes=inputs + [pltpu.VMEM((1, wide), jnp.float32)],
            compiler_params=params,
            cost_estimate=cost,
            name="sinkhorn_last",
        )(*scalars, gap, *slices, k, scale, mrow, bs)[4]

    return first, middle, last


def hop_of(i):
    return (i + 1) // 2 if i % 2 == 0 else -((i + 1) // 2)


def ring_at(place, ranks):
    return jnp.where(place < ranks // 2, 2 * place, 2 * (ranks - 1 - place) + 1)


def match_kernel(place, counts, pairs, bins, row_desc, *refs, ranks, rows, pair_count):
    tables = refs[: ranks // 2]
    chunks = refs[ranks // 2 : ranks // 2 + ranks + 1]
    log_match, row_bins, col_bins, table = refs[ranks // 2 + ranks + 1 :]
    p = pl.program_id(0)
    kp = rows * ranks
    rank = place[0]
    na = counts[pairs[2 * p]]
    nb = counts[pairs[2 * p + 1]]
    away = (((ranks - pair_count) // 2 + p) ^ rank) // 2
    for i in range(ranks // 2):
        @pl.when(away == i)
        def _():
            table[0] = tables[i][lax.rem(p, 2)]
    at = jnp.where(lax.rem(rank, 2) == 0, rank // 2, ranks - 1 - rank // 2)
    offset = pl.multiple_of(rank * rows, rows)
    log_norm = -jnp.log(jnp.full((1, 1), na + nb, jnp.int32).astype(jnp.float32))
    bin_v = bins[0]
    u = table[0, 0:1, pl.ds(offset, rows)]
    u_bin = table[0, 0:1, kp : kp + 1]
    v_bin = table[0, 1:2, kp : kp + 1]
    lane = lax.broadcasted_iota(jnp.int32, (1, kp), 1)
    row_ok = lane[:, :rows] + offset < na
    row_bins[pl.ds(p, 1), :] = jnp.where(row_ok, bin_v + u + v_bin - log_norm, 0.0)
    col_bins[pl.ds(p, 1), :] = jnp.where(lane < nb, bin_v + u_bin + table[0, 1:2, :kp] - log_norm, 0.0)
    u_tall = [spread(u[:, lanes(i)]) for i in range(rows // LANES)]
    u_tall = u_tall[0] if len(u_tall) == 1 else jnp.concatenate(u_tall, axis=0)
    inside = lax.broadcasted_iota(jnp.int32, (rows, 1), 0) + offset < na
    factor = jnp.bfloat16(row_desc.shape[2] ** (-0.5))
    mine = row_desc[p] * factor
    for i in range(ranks):
        start = pl.multiple_of(ring_at(lax.rem(at + ranks + hop_of(i), ranks), ranks) * rows, rows)
        if i + 1 < ranks:
            desc = chunks[i][p]
        else:
            half = pair_count // 2
            desc = jnp.where(p < half, chunks[i][jnp.minimum(p, half - 1)], chunks[i + 1][jnp.maximum(p - half, 0)])
        s = lax.dot_general(mine, desc, (((1,), (1,)), ((), ())), preferred_element_type=jnp.float32)
        v = table[0, 1:2, pl.ds(start, rows)] - log_norm
        ok = inside & (lane[:, :rows] + start < nb)
        log_match[0, :, pl.ds(start, rows)] = jnp.where(ok, s + u_tall + v, 0.0)


def finish(scalars, row_desc, tables, chunks):
    pair_count, rows, depth = row_desc.shape
    ranks = len(chunks) - 1
    kp = rows * ranks
    smem = pl.BlockSpec(memory_space=pltpu.SMEM)
    vmem = pl.BlockSpec(memory_space=pltpu.VMEM)
    return pl.pallas_call(
        functools.partial(match_kernel, ranks=ranks, rows=rows, pair_count=pair_count),
        grid=(pair_count,),
        out_shape=(
            jax.ShapeDtypeStruct((pair_count, rows, kp), jnp.float32),
            jax.ShapeDtypeStruct((pair_count, rows), jnp.float32),
            jax.ShapeDtypeStruct((pair_count, kp), jnp.float32),
        ),
        in_specs=[smem] * 4 + [vmem] * (1 + len(tables) + len(chunks)),
        out_specs=(
            pl.BlockSpec((1, rows, kp), lambda p: (p, 0, 0)),
            pl.BlockSpec((pair_count, rows), lambda p: (0, 0)),
            pl.BlockSpec((pair_count, kp), lambda p: (0, 0)),
        ),
        scratch_shapes=[pltpu.VMEM((1,) + tables[0].shape[1:], jnp.float32)],
        compiler_params=pltpu.CompilerParams(vmem_limit_bytes=10 << 20),
        name="match",
    )(*scalars, row_desc, *tables, *chunks)


def completed(links, ranks):
    sources = [r for r in range(ranks) if r not in [a for a, _ in links]]
    targets = [r for r in range(ranks) if r not in [b for _, b in links]]
    return links + [(a, b) if a != b else (a, a ^ 1) for a, b in zip(sources, targets)]


def on_device(descriptors, counts, pairs, bin_score):
    local_rows, depth = descriptors.shape[1:]
    ranks = lax.axis_size("row")
    rank = lax.axis_index("row")
    pair_count = pairs.shape[0]
    first = (ranks - pair_count) // 2
    row_desc = descriptors[pairs[:, 0]]
    col_desc = descriptors[pairs[:, 1]]
    both = jnp.stack([row_desc, col_desc], axis=1)

    def for_owner(owner):
        return lax.dynamic_index_in_dim(both, jnp.clip(owner - first, 0, pair_count - 1), 0, keepdims=False)

    messages = [for_owner(rank ^ i) for i in range(ranks)]
    flat, col_desc, messages = lax.optimization_barrier((pairs.reshape(-1), col_desc, messages))
    scalars = (rank[None], counts, flat, bin_score)
    slices = [messages[0]]
    for i in range(1, ranks):
        links = completed([((first + p) ^ i, first + p) for p in range(pair_count)], ranks)
        slices.append(lax.ppermute(messages[i], "row", links))
    ring = list(range(0, ranks, 2)) + list(range(1, ranks, 2))[::-1]
    ahead = [(ring[i], ring[(i + 1) % ranks]) for i in range(ranks)]
    behind = [(b, a) for a, b in ahead]
    chunks = [col_desc]

    def hop(step, fore, back):
        if step == ranks // 2:
            half = pair_count // 2
            fore, back = fore[:half], back[half:]
        fore = lax.ppermute(fore, "row", ahead)
        back = lax.ppermute(back, "row", behind)
        chunks.extend([fore, back])
        return fore, back

    slices, col_desc = lax.optimization_barrier((slices, col_desc))
    first_stage, middle_stage, last_stage = stages(scalars, slices)
    fore, back = hop(1, col_desc, col_desc)
    state = first_stage()
    bs, fore, back = lax.optimization_barrier((state[3], fore, back))
    fore, back = hop(2, fore, back)
    state = middle_stage((*state[:3], bs, state[4]))
    bs, fore, back = lax.optimization_barrier((state[3], fore, back))
    fore, back = hop(3, fore, back)
    pots = last_stage((*state[:3], bs, state[4]))
    pots, fore, back = lax.optimization_barrier((pots, fore, back))
    for step in range(4, ranks // 2 + 1):
        fore, back = hop(step, fore, back)
    other = lax.ppermute(pots, "row", [(r, r ^ 1) for r in range(ranks)])
    odd = lax.rem(rank, 2) == 1
    table = jnp.stack([jnp.where(odd, other, pots), jnp.where(odd, pots, other)])
    tables = [table]
    for i in range(2, ranks, 2):
        links = completed([(first + p, (first + p) ^ i) for p in range(pair_count)], ranks)
        tables.append(lax.ppermute(table, "row", links))
    return finish(scalars, row_desc, tables, chunks)


def solution(mesh):
    return jax.shard_map(
        on_device,
        mesh=mesh,
        in_specs=(P("pair", "row", None), P("pair"), P("pair", None), P()),
        out_specs=(P("pair", "row", None), P("pair", "row"), P("pair", None)),
        check_vma=False,
    )
```
